32 devices in a mesh: expert: 4 (over y, x), shard: 8 (over z, core).
Axes of the slice: x: 2, y: 2, z: 4, core: 2. Of those that a mesh axis runs over, the one named last changes fastest.
Arguments:
- tokens: bfloat16 [256, 6144], P(('expert', 'shard')), may hold values from -6 to 6
- norm_gain: float32 [6144], replicated, may hold values from 0.5 to 1.5
- routes: int32 [256, 2], P(('expert', 'shard')), may hold values from 0 to 3, all different within a row; in each aligned block of 8 rows (0 to 7, 8 to 15, ...) at most 4 rows name the same one
- gate_weights: float32 [256, 2], P(('expert', 'shard')), may hold values from 0.2 to 1
- capacity: int32 [4], replicated, may hold values from 2 to 4
- w_gate: bfloat16 [4, 6144, 8192], P('expert', None, 'shard'), may hold values from -0.078125 to 0.078125
- w_up: bfloat16 [4, 6144, 8192], P('expert', None, 'shard'), may hold values from -0.078125 to 0.078125
- w_down: bfloat16 [4, 8192, 6144], P('expert', 'shard'), may hold values from -0.0625 to 0.0625
Outputs:
- mixed_out: bfloat16 [256, 6144], P(('expert', 'shard'))
The draws below stay inside these ranges and needn't reach their ends.
Inputs may be any that keep to these rules, and one draw needn't show every extreme that they name: `routes`: each row names 2 different experts; among the rows of one device no expert is named by more than 4 rows.
All inputs are finite; a program needn't handle non-finite values.
Results may differ from the reference program's by a relative error of at most 0.019.
Values may be sent and summed in bfloat16 or wider, within the bound.
No kernel may reach another device: no remote copies, remote signals or barrier semaphores. Data moves between devices by JAX's collectives and lax.ppermute only.
A program may use at most 128 MiB of HBM per device.

```python
import math
import jax
import jax.numpy as jnp
import numpy as np
from jax import lax

D = 6144
FF = 8192
TOPK = 2
TOK_DEV = 8
EXPERTS = 4
MOST = 4
TOKENS = 256
N_SHARD = 8


def draw_capacity(key, part):
    drawn_caps = jax.random.randint(key, (EXPERTS,), MOST // 2, MOST + 1, dtype=jnp.int32)
    chosen = jax.random.randint(jax.random.fold_in(key, 7), (), 0, EXPERTS, dtype=jnp.int32)
    return jnp.where(jnp.arange(EXPERTS, dtype=jnp.int32) == chosen, MOST, drawn_caps).astype(jnp.int32)


def levels(rng, extent, shards, low, high):
    level, own = 1.0, jax.random.fold_in(rng, 6)
    for dim, blocks in shards:
        draws = jnp.exp(jax.random.uniform(jax.random.fold_in(own, dim), (blocks,), jnp.float32, low / len(shards), high / len(shards)))
        level = level * jnp.repeat(draws, extent[dim] // blocks).reshape([-1 if axis == dim else 1 for axis in range(len(extent))])
    return level


def assign_block(own_key, own, number, rows, amount, top, bound, skew):
    order = jax.random.permutation(own_key, amount)
    packed, usual = portions_of(amount, rows * top, bound, skew, True), portions_of(amount, rows * top, bound, skew, False)
    places = jnp.arange(amount)

    def named(tallies, offset_by):
        used = int((tallies > 0).sum())
        fixed = max(1, used // 4)
        passed = fixed + (places - fixed + offset_by * (used - fixed)) % max(1, amount - fixed)
        return jnp.zeros((amount,), jnp.int32).at[order[jnp.where(places < fixed, places, passed)]].set(jnp.asarray(tallies, jnp.int32))

    tallies = jnp.where(number % 4 == 0, named(packed, number // 4), named(usual, number - number // 4 - 1))
    mixed = jax.random.permutation(jax.random.fold_in(own, 3), amount)
    giver, sink = mixed[0:amount // 2 * 2:2], mixed[1:amount // 2 * 2:2]
    margin = jnp.minimum(tallies[giver] - 1, bound - tallies[sink]) // 2
    margin = jnp.where((giver == order[0]) | (sink == order[0]) | (tallies[sink] == 0), 0, jnp.maximum(margin, 0))
    passed = jax.random.randint(jax.random.fold_in(own, 4), (amount // 2,), 0, 1 << 20) % (margin + 1)
    tallies = tallies.at[giver].add(-passed).at[sink].add(passed)
    members = jnp.searchsorted(jnp.cumsum(tallies), jnp.arange(rows * top), side="right").astype(jnp.int32)
    listing = members.reshape(top, rows).T
    listing = listing[jax.random.permutation(jax.random.fold_in(own, 1), rows)]
    offset_by = jax.random.randint(jax.random.fold_in(own, 2), (rows, 1), 0, top)
    return jnp.take_along_axis(listing, (jnp.arange(top)[None, :] + offset_by) % top, axis=1)


def portions_of(amount, total, bound, lean, full):
    weights = [(1 << 20) // math.isqrt(standing ** lean) + 1 for standing in range(1, amount + 1)]
    largest = bound if full else min(bound, max(-(-total // amount), total * weights[0] // sum(weights)))
    least = 1 if total - largest >= amount - 1 else 0
    holding, surplus = [largest] + [least] * (amount - 1), total - largest - least * (amount - 1)
    while surplus > 0:
        free = [i for i in range(1, amount) if holding[i] < largest] or [i for i in range(1, amount) if holding[i] < bound]
        mass, budget = sum([weights[i] for i in free]), surplus
        for i in free:
            extra = min(bound - holding[i], max(1, budget * weights[i] // mass), surplus)
            holding[i] = holding[i] + extra
            surplus = surplus - extra
    return np.array(holding)


def centred(key, dims, scale, limit, cuts=(), held_as=jnp.bfloat16):
    gain = levels(key, dims, cuts, -0.22, 0.18) if cuts else 1.0
    result = jax.random.normal(key, dims, jnp.float32) * scale * gain
    return jnp.minimum(jnp.maximum(result, -limit), limit).astype(held_as)


def setup_inputs(seed: int = 0) -> dict:
    keys = jax.random.split(jax.random.key(seed), 9)
    tokens = centred(keys[0], (TOKENS, D), 1.0, 6.0, ((0, 32),))
    norm_gain = jnp.clip(1.0 + 0.1 * jax.random.normal(keys[1], (D,), jnp.float32), 0.5, 1.5)
    routes_keys = jax.random.split(jax.random.fold_in(keys[2], 1), TOKENS // TOK_DEV)
    routes_turns = jax.random.permutation(jax.random.fold_in(keys[2], 3), TOKENS // TOK_DEV)
    routes = jax.vmap(lambda own, number: assign_block(jax.random.fold_in(keys[2], 2), own, number, TOK_DEV, EXPERTS, TOPK, MOST, 2))(routes_keys, routes_turns).reshape((TOKENS, TOPK))
    gate_weights = jnp.clip(jnp.exp(math.log(1.0) - 1.609438 * jax.random.uniform(keys[3], (TOKENS, TOPK), jnp.float32) ** levels(keys[3], (TOKENS, TOPK), ((0, 32),), -0.2, 0.2)), 0.2, 1.0)
    capacity = draw_capacity(jax.random.fold_in(keys[8], 71), 0)
    w_gate = centred(keys[5], (EXPERTS, D, FF), D ** -0.5, 0.078125, ((0, 4), (2, 8)))
    w_up = centred(keys[6], (EXPERTS, D, FF), D ** -0.5, 0.078125, ((0, 4), (2, 8)))
    w_down = centred(keys[7], (EXPERTS, FF, D), FF ** -0.5, 0.0625, ((0, 4), (1, 8)))
    return {"tokens": tokens, "norm_gain": norm_gain, "routes": routes, "gate_weights": gate_weights, "capacity": capacity, "w_gate": w_gate, "w_up": w_up, "w_down": w_down}


def rms_norm(tokens, norm_gain):
    widened = tokens.astype(jnp.float32)
    mean_square = lax.optimization_barrier(jnp.mean(widened * widened, axis=-1, keepdims=True))
    return (widened * lax.rsqrt(mean_square + 1e-05) * norm_gain).astype(jnp.bfloat16)

def slot_ranks(blocked):
    equal_ids = blocked[:, :, None, :, None] == blocked[:, None, :, None, :]
    shared = jnp.any(equal_ids, axis=4).astype(jnp.int32)
    per_block = blocked.shape[1]
    positions = jnp.arange(per_block, dtype=jnp.int32)
    earlier = (positions[None, :] < positions[:, None]).astype(jnp.int32)
    return lax.optimization_barrier(jnp.sum(shared * earlier[None, :, :, None], axis=2)).astype(jnp.int32)

def expert_apply(buffer, gate_proj, up_proj, down_proj):
    gate_val = jnp.dot(buffer, gate_proj, preferred_element_type=jnp.float32)
    up_val = jnp.dot(buffer, up_proj, preferred_element_type=jnp.float32)
    hidden = (jax.nn.silu(gate_val) * up_val).astype(jnp.bfloat16)
    hidden_width = FF // N_SHARD

    def add_shard(running, shard_idx):
        start_col = (shard_idx * hidden_width).astype(jnp.int32)
        hidden_part = lax.dynamic_slice_in_dim(hidden, start_col, hidden_width, 1)
        down_part = lax.dynamic_slice_in_dim(down_proj, start_col, hidden_width, 0)
        rounded = jnp.dot(hidden_part, down_part, preferred_element_type=jnp.float32).astype(jnp.bfloat16)
        rounded = lax.optimization_barrier(rounded)
        return (running + rounded.astype(jnp.float32), None)
    initial = jnp.zeros((buffer.shape[0], down_proj.shape[1]), jnp.float32)
    running, _ = lax.scan(add_shard, initial, jnp.arange(N_SHARD, dtype=jnp.int32))
    return running.astype(jnp.bfloat16)

def reference(tokens, norm_gain, routes, gate_weights, capacity, w_gate, w_up, w_down):
    normed = rms_norm(tokens, norm_gain)
    nblocks = TOKENS // TOK_DEV
    slot_rank = slot_ranks(routes.reshape(nblocks, TOK_DEV, TOPK)).reshape(TOKENS, TOPK)
    kept_mask = slot_rank < capacity[routes]
    block_ids = (jnp.arange(TOKENS, dtype=jnp.int32) // TOK_DEV)[:, None]
    slot_index = (block_ids * MOST + slot_rank).astype(jnp.int32)
    dump_row = nblocks * MOST
    mixed_out = jnp.zeros((TOKENS, D), jnp.float32)
    for expert_idx in range(EXPERTS):
        routed_mask = kept_mask & (routes == expert_idx)
        dest_rows = jnp.where(routed_mask, slot_index, dump_row).astype(jnp.int32)
        buffer = jnp.zeros((dump_row + 1, D), jnp.bfloat16)
        for slot_k in range(TOPK):
            buffer = buffer.at[dest_rows[:, slot_k]].set(normed)
        expert_out = expert_apply(buffer, w_gate[expert_idx], w_up[expert_idx], w_down[expert_idx])
        for slot_k in range(TOPK):
            taken = expert_out[dest_rows[:, slot_k]].astype(jnp.float32)
            weighted = gate_weights[:, slot_k:slot_k + 1] * taken
            mixed_out = mixed_out + jnp.where(routed_mask[:, slot_k:slot_k + 1], weighted, jnp.float32(0.0))
    return mixed_out.astype(jnp.bfloat16)
```

```python
import jax
import jax.numpy as jnp
from jax import lax
from jax.sharding import Mesh, PartitionSpec as P
import jax.experimental.pallas as pl
import jax.experimental.pallas.tpu as pltpu

CORES = 2
MIB = 1 << 20
LANES = 128
MOST_VMEM = 67035136
PARTS_IN = 1
CUTS = (6,)
TILE = 256
MIX_PARTS = 6
VMEM = pltpu.VMEM
SMEM = pltpu.SMEM


def whole(space=VMEM):
    return pl.BlockSpec(memory_space=space)


def params(mib):
    return pltpu.CompilerParams(vmem_limit_bytes=mib * MIB)


def home_kernel(depth, cap_hbm, tok_hbm, gain_hbm, routes_hbm, gates_hbm, *refs):
    meta_ref, cap_ref, tok_ref, gain_ref, routes_ref, gates_ref, sem = refs[-7:]
    exts = refs[:-7]
    small = [(cap_hbm, cap_ref), (routes_hbm, routes_ref), (gates_hbm, gates_ref)]
    pairs = small + [(tok_hbm, tok_ref), (gain_hbm, gain_ref)]
    copies = [pltpu.make_async_copy(src, dst, sem.at[i]) for i, (src, dst) in enumerate(pairs)]
    for c in copies:
        c.start()
    tok, width = tok_ref.shape
    row = lax.broadcasted_iota(jnp.int32, (tok, tok), 0)
    col = lax.broadcasted_iota(jnp.int32, (tok, tok), 1)
    for c in copies[:3]:
        c.wait()

    def upright(line):
        return jnp.sum(jnp.where(row == col, line, 0.0), axis=1, keepdims=True)

    across = routes_ref[...].astype(jnp.float32)
    codes = []
    for k in range(2):
        mine = upright(across[k:k + 1, :])
        same = (across[0:1, :] == mine) | (across[1:2, :] == mine)
        rank = jnp.sum(jnp.where(same & (col < row), 1.0, 0.0), axis=1, keepdims=True)
        cap = jnp.zeros_like(mine)
        for e in range(cap_ref.shape[0]):
            cap = jnp.where(mine == e, cap_ref[e].astype(jnp.float32), cap)
        codes.append(jnp.where(rank < cap, mine * depth + rank, -1.0))
    lane = lax.broadcasted_iota(jnp.int32, (tok, LANES), 1)
    code = jnp.where(lane == 0, codes[0], jnp.where(lane == 1, codes[1], 0.0))
    gate = [upright(gates_ref[k:k + 1, :]) for k in range(2)]
    meta_ref[...] = code + jnp.where(lane == 2, gate[0], jnp.where(lane == 3, gate[1], 0.0))
    step = width // len(exts)
    exts[0][:, step:] = code.astype(jnp.bfloat16)
    for c in copies[3:]:
        c.wait()
    wide = tok_ref[...].astype(jnp.float32)
    scale = lax.rsqrt(jnp.mean(wide * wide, axis=-1, keepdims=True) + 1e-05)
    normed = (wide * scale * gain_ref[...]).astype(jnp.bfloat16)
    for i, ext_ref in enumerate(exts):
        ext_ref[:, :step] = normed[:, i * step:(i + 1) * step]


def pack_kernel(depth, zs, first, *refs):
    sources = zs if first else 2 * zs
    experts = len(refs) - sources
    me = lax.axis_index("expert")
    ins, data, outs = refs[:zs], refs[sources - zs:sources], refs[sources:]
    tok = ins[0].shape[0]
    width = outs[0].shape[1]
    rows = experts * zs * depth
    picks = []
    row = lax.broadcasted_iota(jnp.int32, (tok, rows), 1)
    k, o, slot = row // (zs * depth), (row // depth) % zs, row % depth
    target = slot
    for i in range(experts):
        target = jnp.where(k == i, slot + (me ^ i) * depth, target)
    target = target.astype(jnp.float32)
    for i in range(zs):
        code = ins[i][:, ins[i].shape[1] - LANES:].astype(jnp.float32)
        hit = (code[:, 0:1] == target) | (code[:, 1:2] == target)
        picks.append(jnp.where(hit & (o == i), 1.0, 0.0))
    pick = jnp.concatenate(picks, axis=0).T.astype(jnp.bfloat16)
    normed = jnp.concatenate([r[:, :width].astype(jnp.float32) for r in data], axis=0).astype(jnp.bfloat16)
    packed = jnp.dot(pick, normed, preferred_element_type=jnp.float32).astype(jnp.bfloat16)
    step = zs * depth
    for i in range(experts):
        outs[i][...] = packed[i * step:(i + 1) * step]


def up_kernel(zs, depth, part, parts, *refs):
    experts = lax.axis_size("expert")
    blocks, (gate_ref, up_ref), refs = refs[:CORES * experts], refs[CORES * experts:CORES * experts + 2], refs[CORES * experts + 2:]
    before = ()
    if part:
        before, refs = refs[:2], refs[2:]
    step, width = blocks[0].shape
    outs = refs[:-1] if part < parts - 1 else refs[:-2]
    x_ref = refs[len(outs)]
    rows = x_ref.shape[0]
    for i, r in enumerate(blocks):
        x_ref[i * step:(i + 1) * step, :] = r[...]
    tile = 256
    span = slice(part * width, (part + 1) * width)
    for n in range(gate_ref.shape[1] // tile):
        cols = slice(n * tile, (n + 1) * tile)
        g = jnp.dot(x_ref[...], gate_ref[span, cols], preferred_element_type=jnp.float32)
        u = jnp.dot(x_ref[...], up_ref[span, cols], preferred_element_type=jnp.float32)
        if part:
            g = g + before[0][:, cols]
            u = u + before[1][:, cols]
        if part < parts - 1:
            outs[0][:, cols] = g
            outs[1][:, cols] = u
        else:
            refs[-1][:, cols] = (g / (1.0 + jnp.exp(-g)) * u).astype(jnp.bfloat16)
    if part < parts - 1:
        return
    hid_ref, h_ref = outs[0], refs[-1]
    chip, me = lax.axis_index("chip"), lax.axis_index("expert")
    row = lax.broadcasted_iota(jnp.int32, (rows, rows), 0)
    col = lax.broadcasted_iota(jnp.int32, (rows, rows), 1)
    slot, z = row % depth, (row // depth) % zs
    e, side = (row // (depth * zs)) % experts, row // (depth * zs * experts)
    block = jnp.zeros_like(e)
    for i in range(experts):
        block = jnp.where(e == (me ^ i), i, block)
    source = ((side * experts + block) * zs + (z ^ chip)) * depth + slot
    order = jnp.where(source == col, 1.0, 0.0).astype(jnp.bfloat16)
    hid_ref[...] = jnp.dot(order, h_ref[...], preferred_element_type=jnp.float32).astype(jnp.bfloat16)


def down_kernel(start, hid_ref, down_ref, kept_ref, sent_ref):
    mine, span = kept_ref.shape
    for n in range(span // TILE):
        cols = slice(start + n * TILE, start + (n + 1) * TILE)
        d = jnp.dot(hid_ref[...], down_ref[:, cols], preferred_element_type=jnp.float32)
        kept_ref[:, n * TILE:(n + 1) * TILE] = d[:mine]
        sent_ref[:, n * TILE:(n + 1) * TILE] = d[mine:].astype(jnp.bfloat16)


def join_kernel(*refs):
    out_ref = refs[-1]
    blocks, depth, width = out_ref.shape
    start = 0
    for kept_ref, sent_ref in zip(refs[:-1:2], refs[1:-1:2]):
        cols = slice(start, start + kept_ref.shape[1])
        both = kept_ref[...] + sent_ref[...].astype(jnp.float32)
        for b in range(blocks):
            out_ref[b, :, cols] = both[b * depth:(b + 1) * depth].astype(jnp.bfloat16)
        start = cols.stop


def mix_kernel(meta_ref, parts_ref, out_ref):
    experts, zs, depth, width = parts_ref.shape
    meta = meta_ref[...]
    weights = []
    for target in range(experts * depth):
        w = jnp.where(meta[:, 1:2] == target, meta[:, 3:4], 0.0)
        weights.append(jnp.where(meta[:, 0:1] == target, meta[:, 2:3], w))
    step = width // MIX_PARTS
    for c in range(MIX_PARTS):
        cols = slice(c * step, (c + 1) * step)
        mixed = jnp.zeros((out_ref.shape[0], step), jnp.float32)
        for e in range(experts):
            total = parts_ref[e, 0, :, cols].astype(jnp.float32)
            for z in range(1, zs):
                total = total + parts_ref[e, z, :, cols].astype(jnp.float32)
            total = total.astype(jnp.bfloat16).astype(jnp.float32)
            for k in range(depth):
                mixed = mixed + weights[e * depth + k] * total[k:k + 1, :]
        out_ref[:, cols] = mixed.astype(jnp.bfloat16)


def flips(count):
    masks = [count - 1] if count > 1 else []
    bit = 1
    while 2 * bit < count:
        masks.append(bit)
        bit *= 2
    if bit * 2 != count and count > 1:
        raise ValueError("axis size")
    return masks


def flip(value, axis, mask):
    return lax.ppermute(value, axis, [(i, i ^ mask) for i in range(lax.axis_size(axis))])


def on_device(tokens, norm_gain, routes, gate_weights, capacity, w_gate, w_up, w_down):
    experts, zs = lax.axis_size("expert"), lax.axis_size("chip")
    tok, width = tokens.shape
    hidden = w_gate.shape[2]
    depth = max(tok // 2, tok * routes.shape[1] // capacity.shape[0])
    swap = lambda v: flip(v, "core", 1)
    rows = CORES * experts * zs * depth
    f32, bf16 = jnp.float32, jnp.bfloat16
    scope = jax.named_scope

    part = width // PARTS_IN
    sizes = [part + LANES] + [part] * (PARTS_IN - 1)
    *exts, meta = pl.pallas_call(
        lambda *r: home_kernel(depth, *r),
        out_shape=[VMEM((tok, n), bf16) for n in sizes] + [VMEM((tok, LANES), f32)],
        in_specs=[whole(pl.ANY)] * 5,
        out_specs=[whole()] * (PARTS_IN + 1),
        scratch_shapes=[
            SMEM(capacity.shape, jnp.int32),
            VMEM((tok, width), bf16),
            VMEM((1, width), f32),
            VMEM((2, tok), jnp.int32),
            VMEM((2, tok), f32),
            pltpu.SemaphoreType.DMA((5,)),
        ],
        compiler_params=pltpu.CompilerParams(vmem_limit_bytes=MOST_VMEM - tok * (2 * (width + LANES) + 4 * LANES)),
        name="home",
    )(capacity, tokens, norm_gain.reshape(1, width), routes.T, gate_weights.T)

    gathered = []
    for i in range(PARTS_IN):
        near = {0: exts[i]}
        for mask in flips(zs):
            for o in list(near):
                near[o ^ mask] = flip(near[o], "chip", mask)
        gathered.append([near[o] for o in range(zs)])
    acc = ()
    for i in range(PARTS_IN):
        first = i == 0
        sources = gathered[0] + ([] if first else gathered[i])
        packed = pl.pallas_call(
            lambda *r, first=first: pack_kernel(depth, zs, first, *r),
            out_shape=[jax.ShapeDtypeStruct((zs * depth, part), bf16)] * experts,
            in_specs=[whole()] * len(sources),
            out_specs=[whole()] * experts,
            compiler_params=params(8),
            cost_estimate=pl.CostEstimate(flops=10**11 if first else 10**6, bytes_accessed=0, transcendentals=0),
            name=f"pack_{i}",
        )(*sources)
        arrived = [packed[0]] + [flip(packed[k], "expert", k) for k in range(1, experts)]
        theirs = [swap(v) for v in arrived]
        last = i == PARTS_IN - 1
        total = jax.ShapeDtypeStruct((rows, hidden), f32)
        scratch = [VMEM((rows, part), bf16)] + ([VMEM((rows, hidden), bf16)] if last else [])
        acc = pl.pallas_call(
            lambda *r, i=i: up_kernel(zs, depth, i, PARTS_IN, *r),
            out_shape=[jax.ShapeDtypeStruct((rows, hidden), bf16)] if last else [total, total],
            in_specs=[whole()] * (CORES * experts + 2 + len(acc)),
            out_specs=[whole()] * (1 if last else 2),
            scratch_shapes=scratch,
            compiler_params=params(10 if rows <= 128 else 22),
            name=f"up_{i}",
        )(*arrived, *theirs, w_gate[0], w_up[0], *acc)
    hid = acc[0]
    mine = rows // CORES
    tiles = width // TILE
    bounds = [0, *[tiles * k // 8 * TILE for k in CUTS], width]
    halves = []
    for j, (start, stop) in enumerate(zip(bounds[:-1], bounds[1:])):
        kept, sent = pl.pallas_call(
            lambda *r, start=start: down_kernel(start, *r),
            out_shape=[jax.ShapeDtypeStruct((mine, stop - start), dtype) for dtype in (f32, bf16)],
            in_specs=[whole(), whole()],
            out_specs=[whole()] * 2,
            compiler_params=params(8),
            cost_estimate=pl.CostEstimate(flops=4 * mine * (stop - start) * hidden, bytes_accessed=0, transcendentals=0),
            name=f"down_{j}",
        )(hid, w_down[0])
        halves += [kept, swap(sent)]
    partial = pl.pallas_call(
        join_kernel,
        out_shape=jax.ShapeDtypeStruct((experts * zs, depth, width), bf16),
        in_specs=[whole()] * len(halves),
        out_specs=whole(),
        compiler_params=params(4 if mine <= 64 else 30),
        name="join",
    )(*halves)
    pieces = lax.all_to_all(partial, ("expert", "chip"), split_axis=0, concat_axis=0, tiled=True)
    return pl.pallas_call(
        mix_kernel,
        out_shape=jax.ShapeDtypeStruct((tok, width), bf16),
        in_specs=[whole()] * 2,
        out_specs=whole(),
        compiler_params=params(16),
        name="mix",
    )(meta, pieces.reshape(experts, zs, depth, width))


def solution(mesh):
    experts, shards = mesh.shape["expert"], mesh.shape["shard"]
    devices = mesh.devices.reshape(experts, shards // CORES, CORES)
    split = Mesh(devices, ("expert", "chip", "core"))
    everywhere = P(("expert", "chip", "core"), None)
    columns = P("expert", None, ("chip", "core"))
    in_specs = (
        everywhere, P(), everywhere, everywhere, P(),
        columns, columns, P("expert", ("chip", "core"), None),
    )
    step = jax.shard_map(on_device, mesh=split, in_specs=in_specs, out_specs=everywhere, check_vma=False)
    return step
```

```python
import jax
import jax.numpy as jnp
from jax import lax
from jax.sharding import Mesh, PartitionSpec as P
import jax.experimental.pallas as pl
import jax.experimental.pallas.tpu as pltpu

CORES = 2
MIB = 1 << 20
LANES = 128
MOST_VMEM = 67035136
CUTS = (6,)
TILE = 256
MIX_PARTS = 6
VMEM = pltpu.VMEM
SMEM = pltpu.SMEM


def whole(space=VMEM):
    return pl.BlockSpec(memory_space=space)


def params(mib):
    return pltpu.CompilerParams(vmem_limit_bytes=mib * MIB)


def home_kernel(depth, cap_hbm, tok_hbm, gain_hbm, routes_hbm, gates_hbm, *refs):
    ext_ref, meta_ref, cap_ref, tok_ref, gain_ref, routes_ref, gates_ref, sem = refs
    small = [(cap_hbm, cap_ref), (routes_hbm, routes_ref), (gates_hbm, gates_ref)]
    pairs = small + [(tok_hbm, tok_ref), (gain_hbm, gain_ref)]
    copies = [pltpu.make_async_copy(src, dst, sem.at[i]) for i, (src, dst) in enumerate(pairs)]
    for c in copies:
        c.start()
    tok, width = tok_ref.shape
    row = lax.broadcasted_iota(jnp.int32, (tok, tok), 0)
    col = lax.broadcasted_iota(jnp.int32, (tok, tok), 1)
    for c in copies[:3]:
        c.wait()

    def upright(line):
        return jnp.sum(jnp.where(row == col, line, 0.0), axis=1, keepdims=True)

    across = routes_ref[...].astype(jnp.float32)
    codes = []
    for k in range(2):
        mine = upright(across[k:k + 1, :])
        same = (across[0:1, :] == mine) | (across[1:2, :] == mine)
        rank = jnp.sum(jnp.where(same & (col < row), 1.0, 0.0), axis=1, keepdims=True)
        cap = jnp.zeros_like(mine)
        for e in range(cap_ref.shape[0]):
            cap = jnp.where(mine == e, cap_ref[e].astype(jnp.float32), cap)
        codes.append(jnp.where(rank < cap, mine * depth + rank, -1.0))
    lane = lax.broadcasted_iota(jnp.int32, (tok, LANES), 1)
    code = jnp.where(lane == 0, codes[0], jnp.where(lane == 1, codes[1], 0.0))
    gate = [upright(gates_ref[k:k + 1, :]) for k in range(2)]
    meta_ref[...] = code + jnp.where(lane == 2, gate[0], jnp.where(lane == 3, gate[1], 0.0))
    ext_ref[:, width:] = code.astype(jnp.bfloat16)
    for c in copies[3:]:
        c.wait()
    wide = tok_ref[...].astype(jnp.float32)
    scale = lax.rsqrt(jnp.mean(wide * wide, axis=-1, keepdims=True) + 1e-05)
    ext_ref[:, :width] = (wide * scale * gain_ref[...]).astype(jnp.bfloat16)


def pack_kernel(depth, zs, *refs):
    experts = len(refs) - zs
    me = lax.axis_index("expert")
    ins, outs = refs[:zs], refs[zs:]
    tok = ins[0].shape[0]
    width = outs[0].shape[1]
    rows = experts * zs * depth
    picks = []
    row = lax.broadcasted_iota(jnp.int32, (tok, rows), 1)
    k, o, slot = row // (zs * depth), (row // depth) % zs, row % depth
    target = slot
    for i in range(experts):
        target = jnp.where(k == i, slot + (me ^ i) * depth, target)
    target = target.astype(jnp.float32)
    for i in range(zs):
        code = ins[i][:, ins[i].shape[1] - LANES:].astype(jnp.float32)
        hit = (code[:, 0:1] == target) | (code[:, 1:2] == target)
        picks.append(jnp.where(hit & (o == i), 1.0, 0.0))
    pick = jnp.concatenate(picks, axis=0).T.astype(jnp.bfloat16)
    normed = jnp.concatenate([r[:, :width].astype(jnp.float32) for r in ins], axis=0).astype(jnp.bfloat16)
    packed = jnp.dot(pick, normed, preferred_element_type=jnp.float32).astype(jnp.bfloat16)
    step = zs * depth
    for i in range(experts):
        outs[i][...] = packed[i * step:(i + 1) * step]


def up_kernel(groups, depth, *refs):
    gate_ref, up_ref, hid_ref, x_ref, h_ref = refs[-5:]
    blocks = refs[:-5]
    rows = x_ref.shape[0]
    start = 0
    for r in blocks:
        x_ref[start:start + r.shape[0], :] = r[...]
        start += r.shape[0]
    for n in range(gate_ref.shape[1] // TILE):
        cols = slice(n * TILE, (n + 1) * TILE)
        g = jnp.dot(x_ref[...], gate_ref[:, cols], preferred_element_type=jnp.float32)
        u = jnp.dot(x_ref[...], up_ref[:, cols], preferred_element_type=jnp.float32)
        h_ref[:, cols] = (g / (1.0 + jnp.exp(-g)) * u).astype(jnp.bfloat16)
    experts, zs = lax.axis_size("expert"), lax.axis_size("chip")
    chip, me = lax.axis_index("chip"), lax.axis_index("expert")
    row = lax.broadcasted_iota(jnp.int32, (rows, rows), 0)
    col = lax.broadcasted_iota(jnp.int32, (rows, rows), 1)
    slot, z = row % depth, (row // depth) % zs
    e, side = (row // (depth * zs)) % experts, row // (depth * zs * experts)
    block = jnp.zeros_like(e)
    for i in range(experts):
        block = jnp.where(e == (me ^ i), i, block)
    offset = z ^ chip
    source, start = jnp.zeros_like(e), 0
    for group in groups:
        for i, o in enumerate(group):
            place = start + (block * len(group) + i) * depth + slot
            source = jnp.where(offset == o, place, source)
        start += experts * len(group) * depth
    source = source + side * (rows // CORES)
    order = jnp.where(source == col, 1.0, 0.0).astype(jnp.bfloat16)
    hid_ref[...] = jnp.dot(order, h_ref[...], preferred_element_type=jnp.float32).astype(jnp.bfloat16)


def down_kernel(start, hid_ref, down_ref, kept_ref, sent_ref):
    mine, span = kept_ref.shape
    for n in range(span // TILE):
        cols = slice(start + n * TILE, start + (n + 1) * TILE)
        d = jnp.dot(hid_ref[...], down_ref[:, cols], preferred_element_type=jnp.float32)
        kept_ref[:, n * TILE:(n + 1) * TILE] = d[:mine]
        sent_ref[:, n * TILE:(n + 1) * TILE] = d[mine:].astype(jnp.bfloat16)


def join_kernel(*refs):
    out_ref = refs[-1]
    blocks, depth, _ = out_ref.shape
    start = 0
    for kept_ref, sent_ref in zip(refs[:-1:2], refs[1:-1:2]):
        cols = slice(start, start + kept_ref.shape[1])
        both = kept_ref[...] + sent_ref[...].astype(jnp.float32)
        for b in range(blocks):
            out_ref[b, :, cols] = both[b * depth:(b + 1) * depth].astype(jnp.bfloat16)
        start = cols.stop


def mix_kernel(meta_ref, parts_ref, out_ref):
    experts, zs, depth, width = parts_ref.shape
    meta = meta_ref[...]
    weights = []
    for target in range(experts * depth):
        w = jnp.where(meta[:, 1:2] == target, meta[:, 3:4], 0.0)
        weights.append(jnp.where(meta[:, 0:1] == target, meta[:, 2:3], w))
    step = width // MIX_PARTS
    for c in range(MIX_PARTS):
        cols = slice(c * step, (c + 1) * step)
        mixed = jnp.zeros((out_ref.shape[0], step), jnp.float32)
        for e in range(experts):
            total = parts_ref[e, 0, :, cols].astype(jnp.float32)
            for z in range(1, zs):
                total = total + parts_ref[e, z, :, cols].astype(jnp.float32)
            total = total.astype(jnp.bfloat16).astype(jnp.float32)
            for k in range(depth):
                mixed = mixed + weights[e * depth + k] * total[k:k + 1, :]
        out_ref[:, cols] = mixed.astype(jnp.bfloat16)


def flips(count):
    masks = [count - 1] if count > 1 else []
    bit = 1
    while 2 * bit < count:
        masks.append(bit)
        bit *= 2
    if bit * 2 != count and count > 1:
        raise ValueError("axis size")
    return masks


def flip(value, axis, mask):
    return lax.ppermute(value, axis, [(i, i ^ mask) for i in range(lax.axis_size(axis))])


def grouped(groups):
    early = sum(groups[:-1], [])
    return [early, groups[-1]]


def on_device(tokens, norm_gain, routes, gate_weights, capacity, w_gate, w_up, w_down):
    experts, zs = lax.axis_size("expert"), lax.axis_size("chip")
    tok, width = tokens.shape
    hidden = w_gate.shape[2]
    depth = max(tok // 2, tok * routes.shape[1] // capacity.shape[0])
    swap = lambda v: flip(v, "core", 1)
    rows = CORES * experts * zs * depth
    f32, bf16 = jnp.float32, jnp.bfloat16

    ext, meta = pl.pallas_call(
        lambda *r: home_kernel(depth, *r),
        out_shape=[VMEM((tok, width + LANES), bf16), VMEM((tok, LANES), f32)],
        in_specs=[whole(pl.ANY)] * 5,
        out_specs=[whole()] * 2,
        scratch_shapes=[
            SMEM(capacity.shape, jnp.int32),
            VMEM((tok, width), bf16),
            VMEM((1, width), f32),
            VMEM((2, tok), jnp.int32),
            VMEM((2, tok), f32),
            pltpu.SemaphoreType.DMA((5,)),
        ],
        compiler_params=pltpu.CompilerParams(vmem_limit_bytes=MOST_VMEM - tok * (2 * (width + LANES) + 4 * LANES)),
        name="home",
    )(capacity, tokens, norm_gain.reshape(1, width), routes.T, gate_weights.T)

    near, groups = {0: ext}, [[0]]
    masks = flips(zs)
    for i, mask in enumerate(masks):
        for o in list(near):
            near[o ^ mask] = flip(near[o], "chip", mask)
        if i >= len(masks) - 2:
            known = sum(groups, [])
            groups.append([o for o in near if o not in known])
    groups = grouped(groups)
    shared = [[], []]
    for g, group in enumerate(groups):
        packed = pl.pallas_call(
            lambda *r, size=len(group): pack_kernel(depth, size, *r),
            out_shape=[jax.ShapeDtypeStruct((len(group) * depth, width), bf16)] * experts,
            in_specs=[whole()] * len(group),
            out_specs=[whole()] * experts,
            compiler_params=params(8),
            cost_estimate=pl.CostEstimate(flops=10**11 if g == 0 else 10**6, bytes_accessed=0, transcendentals=0),
        )(*[near[o] for o in group])
        arrived = [packed[0]]
        for k in range(1, experts):
            arrived.append(flip(packed[k], "expert", k))
        for k in range(experts):
            shared[1].append(swap(arrived[k]))
        shared[0] += arrived
    blocks = shared[0] + shared[1]
    hid = pl.pallas_call(
        lambda *r: up_kernel(groups, depth, *r),
        out_shape=jax.ShapeDtypeStruct((rows, hidden), bf16),
        in_specs=[whole()] * (len(blocks) + 2),
        out_specs=whole(),
        scratch_shapes=[VMEM((rows, width), bf16), VMEM((rows, hidden), bf16)],
        compiler_params=params(10 if rows <= 128 else 22),
        name="up",
    )(*blocks, w_gate[0], w_up[0])

    mine = rows // CORES
    tiles = width // TILE
    bounds = [0, *[tiles * k // 8 * TILE for k in CUTS], width]
    halves = []
    for start, stop in zip(bounds[:-1], bounds[1:]):
        kept, sent = pl.pallas_call(
            lambda *r, start=start: down_kernel(start, *r),
            out_shape=[jax.ShapeDtypeStruct((mine, stop - start), dtype) for dtype in (f32, bf16)],
            in_specs=[whole(), whole()],
            out_specs=[whole()] * 2,
            compiler_params=params(8),
            cost_estimate=pl.CostEstimate(flops=4 * mine * (stop - start) * hidden, bytes_accessed=0, transcendentals=0),
        )(hid, w_down[0])
        halves += [kept, swap(sent)]
    partial = pl.pallas_call(
        join_kernel,
        out_shape=jax.ShapeDtypeStruct((experts * zs, depth, width), bf16),
        in_specs=[whole()] * len(halves),
        out_specs=whole(),
        compiler_params=params(4 if mine <= 64 else 30),
        name="join",
    )(*halves)
    pieces = lax.all_to_all(partial, ("expert", "chip"), split_axis=0, concat_axis=0, tiled=True)
    return pl.pallas_call(
        mix_kernel,
        out_shape=jax.ShapeDtypeStruct((tok, width), bf16),
        in_specs=[whole()] * 2,
        out_specs=whole(),
        compiler_params=params(16),
        name="mix",
    )(meta, pieces.reshape(experts, zs, depth, width))


def solution(mesh):
    experts, shards = mesh.shape["expert"], mesh.shape["shard"]
    devices = mesh.devices.reshape(experts, shards // CORES, CORES)
    split = Mesh(devices, ("expert", "chip", "core"))
    everywhere = P(("expert", "chip", "core"), None)
    columns = P("expert", None, ("chip", "core"))
    in_specs = (
        everywhere, P(), everywhere, everywhere, P(),
        columns, columns, P("expert", ("chip", "core"), None),
    )
    return jax.shard_map(on_device, mesh=split, in_specs=in_specs, out_specs=everywhere, check_vma=False)
```

```python
import jax
import jax.numpy as jnp
from jax import lax
from jax.sharding import Mesh, PartitionSpec as P
import jax.experimental.pallas as pl
import jax.experimental.pallas.tpu as pltpu

CORES = 2
MIB = 1 << 20
LANES = 128
MOST_VMEM = 67035136
CUTS = (6,)
TILE = 512
MIX_PARTS = 6
VMEM = pltpu.VMEM
SMEM = pltpu.SMEM


def whole(space=VMEM):
    return pl.BlockSpec(memory_space=space)


def params(mib):
    return pltpu.CompilerParams(vmem_limit_bytes=mib * MIB)


def home_kernel(depth, cap_hbm, tok_hbm, gain_hbm, routes_hbm, gates_hbm, *refs):
    ext_ref, meta_ref, cap_ref, tok_ref, gain_ref, routes_ref, gates_ref, sem = refs
    small = [(cap_hbm, cap_ref), (routes_hbm, routes_ref), (gates_hbm, gates_ref)]
    pairs = small + [(tok_hbm, tok_ref), (gain_hbm, gain_ref)]
    copies = [pltpu.make_async_copy(src, dst, sem.at[i]) for i, (src, dst) in enumerate(pairs)]
    for c in copies:
        c.start()
    tok, width = tok_ref.shape
    row = lax.broadcasted_iota(jnp.int32, (tok, tok), 0)
    col = lax.broadcasted_iota(jnp.int32, (tok, tok), 1)
    for c in copies[:3]:
        c.wait()

    def upright(line):
        return jnp.sum(jnp.where(row == col, line, 0.0), axis=1, keepdims=True)

    across = routes_ref[...].astype(jnp.float32)
    codes = []
    for k in range(2):
        mine = upright(across[k:k + 1, :])
        same = (across[0:1, :] == mine) | (across[1:2, :] == mine)
        rank = jnp.sum(jnp.where(same & (col < row), 1.0, 0.0), axis=1, keepdims=True)
        cap = jnp.zeros_like(mine)
        for e in range(cap_ref.shape[0]):
            cap = jnp.where(mine == e, cap_ref[e].astype(jnp.float32), cap)
        codes.append(jnp.where(rank < cap, mine * depth + rank, -1.0))
    lane = lax.broadcasted_iota(jnp.int32, (tok, LANES), 1)
    code = jnp.where(lane == 0, codes[0], jnp.where(lane == 1, codes[1], 0.0))
    gate = [upright(gates_ref[k:k + 1, :]) for k in range(2)]
    meta_ref[...] = code + jnp.where(lane == 2, gate[0], jnp.where(lane == 3, gate[1], 0.0))
    ext_ref[:, width:] = code.astype(jnp.bfloat16)
    for c in copies[3:]:
        c.wait()
    wide = tok_ref[...].astype(jnp.float32)
    scale = lax.rsqrt(jnp.mean(wide * wide, axis=-1, keepdims=True) + 1e-05)
    ext_ref[:, :width] = (wide * scale * gain_ref[...]).astype(jnp.bfloat16)


def pack_kernel(depth, zs, *refs):
    experts = len(refs) - zs
    me = lax.axis_index("expert")
    ins, outs = refs[:zs], refs[zs:]
    tok = ins[0].shape[0]
    width = outs[0].shape[1]
    rows = experts * zs * depth
    picks = []
    row = lax.broadcasted_iota(jnp.int32, (tok, rows), 1)
    k, o, slot = row // (zs * depth), (row // depth) % zs, row % depth
    target = slot
    for i in range(experts):
        target = jnp.where(k == i, slot + (me ^ i) * depth, target)
    target = target.astype(jnp.float32)
    for i in range(zs):
        code = ins[i][:, ins[i].shape[1] - LANES:].astype(jnp.float32)
        hit = (code[:, 0:1] == target) | (code[:, 1:2] == target)
        picks.append(jnp.where(hit & (o == i), 1.0, 0.0))
    pick = jnp.concatenate(picks, axis=0).T.astype(jnp.bfloat16)
    normed = jnp.concatenate([r[:, :width].astype(jnp.float32) for r in ins], axis=0).astype(jnp.bfloat16)
    packed = jnp.dot(pick, normed, preferred_element_type=jnp.float32).astype(jnp.bfloat16)
    step = zs * depth
    for i in range(experts):
        outs[i][...] = packed[i * step:(i + 1) * step]


def up_kernel(groups, depth, *refs):
    gate_ref, up_ref, _, hid_ref, x_ref, h_ref = refs[-6:]
    blocks = refs[:-6]
    rows = x_ref.shape[0]
    start = 0
    for r in blocks:
        x_ref[start:start + r.shape[0], :] = r[...]
        start += r.shape[0]
    for n in range(gate_ref.shape[1] // TILE):
        cols = slice(n * TILE, (n + 1) * TILE)
        g = jnp.dot(x_ref[...], gate_ref[:, cols], preferred_element_type=jnp.float32)
        u = jnp.dot(x_ref[...], up_ref[:, cols], preferred_element_type=jnp.float32)
        h_ref[:, cols] = (g / (1.0 + jnp.exp(-g)) * u).astype(jnp.bfloat16)
    experts, zs = lax.axis_size("expert"), lax.axis_size("chip")
    chip, me = lax.axis_index("chip"), lax.axis_index("expert")
    row = lax.broadcasted_iota(jnp.int32, (rows, rows), 0)
    col = lax.broadcasted_iota(jnp.int32, (rows, rows), 1)
    slot, z = row % depth, (row // depth) % zs
    e, side = (row // (depth * zs)) % experts, row // (depth * zs * experts)
    block = jnp.zeros_like(e)
    for i in range(experts):
        block = jnp.where(e == (me ^ i), i, block)
    offset = z ^ chip
    source, start = jnp.zeros_like(e), 0
    for group in groups:
        for i, o in enumerate(group):
            place = start + (block * len(group) + i) * depth + slot
            source = jnp.where(offset == o, place, source)
        start += experts * len(group) * depth
    source = source + side * (rows // CORES)
    order = jnp.where(source == col, 1.0, 0.0).astype(jnp.bfloat16)
    hid_ref[...] = jnp.dot(order, h_ref[...], preferred_element_type=jnp.float32).astype(jnp.bfloat16)


def down_kernel(start, hid_ref, down_ref, kept_ref, sent_ref):
    mine, span = kept_ref.shape
    for n in range(span // TILE):
        cols = slice(start + n * TILE, start + (n + 1) * TILE)
        d = jnp.dot(hid_ref[...], down_ref[:, cols], preferred_element_type=jnp.float32)
        kept_ref[:, n * TILE:(n + 1) * TILE] = d[:mine]
        sent_ref[:, n * TILE:(n + 1) * TILE] = d[mine:].astype(jnp.bfloat16)


def join_kernel(*refs):
    out_ref = refs[-1]
    blocks, depth, _ = out_ref.shape
    start = 0
    for kept_ref, sent_ref in zip(refs[:-1:2], refs[1:-1:2]):
        cols = slice(start, start + kept_ref.shape[1])
        both = kept_ref[...] + sent_ref[...].astype(jnp.float32)
        for b in range(blocks):
            out_ref[b, :, cols] = both[b * depth:(b + 1) * depth].astype(jnp.bfloat16)
        start = cols.stop


def mix_kernel(meta_ref, parts_ref, out_ref):
    experts, zs, depth, width = parts_ref.shape
    meta = meta_ref[...]
    weights = []
    for target in range(experts * depth):
        w = jnp.where(meta[:, 1:2] == target, meta[:, 3:4], 0.0)
        weights.append(jnp.where(meta[:, 0:1] == target, meta[:, 2:3], w))
    step = width // MIX_PARTS
    for c in range(MIX_PARTS):
        cols = slice(c * step, (c + 1) * step)
        mixed = jnp.zeros((out_ref.shape[0], step), jnp.float32)
        for e in range(experts):
            total = parts_ref[e, 0, :, cols].astype(jnp.float32)
            for z in range(1, zs):
                total = total + parts_ref[e, z, :, cols].astype(jnp.float32)
            total = total.astype(jnp.bfloat16).astype(jnp.float32)
            for k in range(depth):
                mixed = mixed + weights[e * depth + k] * total[k:k + 1, :]
        out_ref[:, cols] = mixed.astype(jnp.bfloat16)


def flips(count):
    masks = [count - 1] if count > 1 else []
    bit = 1
    while 2 * bit < count:
        masks.append(bit)
        bit *= 2
    if bit * 2 != count and count > 1:
        raise ValueError("axis size")
    return masks


def flip(value, axis, mask):
    return lax.ppermute(value, axis, [(i, i ^ mask) for i in range(lax.axis_size(axis))])


def grouped(groups):
    early = sum(groups[:-1], [])
    return [early, groups[-1]]


def on_device(tokens, norm_gain, routes, gate_weights, capacity, w_gate, w_up, w_down):
    experts, zs = lax.axis_size("expert"), lax.axis_size("chip")
    tok, width = tokens.shape
    hidden = w_gate.shape[2]
    depth = max(tok // 2, tok * routes.shape[1] // capacity.shape[0])
    swap = lambda v: flip(v, "core", 1)
    rows = CORES * experts * zs * depth
    f32, bf16 = jnp.float32, jnp.bfloat16

    ext, meta = pl.pallas_call(
        lambda *r: home_kernel(depth, *r),
        out_shape=[VMEM((tok, width + LANES), bf16), VMEM((tok, LANES), f32)],
        in_specs=[whole(pl.ANY)] * 5,
        out_specs=[whole()] * 2,
        scratch_shapes=[
            SMEM(capacity.shape, jnp.int32),
            VMEM((tok, width), bf16),
            VMEM((1, width), f32),
            VMEM((2, tok), jnp.int32),
            VMEM((2, tok), f32),
            pltpu.SemaphoreType.DMA((5,)),
        ],
        compiler_params=pltpu.CompilerParams(vmem_limit_bytes=MOST_VMEM - tok * (2 * (width + LANES) + 4 * LANES)),
        name="home",
    )(capacity, tokens, norm_gain.reshape(1, width), routes.T, gate_weights.T)

    near, groups = {0: ext}, [[0]]
    masks = flips(zs)
    for i, mask in enumerate(masks):
        for o in list(near):
            near[o ^ mask] = flip(near[o], "chip", mask)
        if i >= len(masks) - 2:
            known = sum(groups, [])
            groups.append([o for o in near if o not in known])
    groups = grouped(groups)
    shared = [[], []]
    for g, group in enumerate(groups):
        packed = pl.pallas_call(
            lambda *r, size=len(group): pack_kernel(depth, size, *r),
            out_shape=[jax.ShapeDtypeStruct((len(group) * depth, width), bf16)] * experts,
            in_specs=[whole()] * len(group),
            out_specs=[whole()] * experts,
            compiler_params=params(8),
            cost_estimate=pl.CostEstimate(flops=10**11 if g == 0 else 10**6, bytes_accessed=0, transcendentals=0),
        )(*[near[o] for o in group])
        arrived = [packed[0]]
        for k in range(1, experts):
            arrived.append(flip(packed[k], "expert", k))
        for k in range(experts):
            shared[1].append(swap(arrived[k]))
        shared[0] += arrived
    blocks = shared[0] + shared[1]
    hid = pl.pallas_call(
        lambda *r: up_kernel(groups, depth, *r),
        out_shape=jax.ShapeDtypeStruct((rows, hidden), bf16),
        in_specs=[whole()] * (len(blocks) + 2) + [whole(pl.ANY)],
        out_specs=whole(),
        scratch_shapes=[VMEM((rows, width), bf16), VMEM((rows, hidden), bf16)],
        compiler_params=params(10 if rows <= 128 else 22),
        name="up",
    )(*blocks, w_gate[0], w_up[0], w_down[0])

    mine = rows // CORES
    tiles = width // TILE
    bounds = [0, *[tiles * k // 8 * TILE for k in CUTS], width]
    halves = []
    for start, stop in zip(bounds[:-1], bounds[1:]):
        kept, sent = pl.pallas_call(
            lambda *r, start=start: down_kernel(start, *r),
            out_shape=[jax.ShapeDtypeStruct((mine, stop - start), dtype) for dtype in (f32, bf16)],
            in_specs=[whole(), whole()],
            out_specs=[whole()] * 2,
            compiler_params=params(8),
            cost_estimate=pl.CostEstimate(flops=4 * mine * (stop - start) * hidden, bytes_accessed=0, transcendentals=0),
        )(hid, w_down[0])
        halves += [kept, swap(sent)]
    partial = pl.pallas_call(
        join_kernel,
        out_shape=jax.ShapeDtypeStruct((experts * zs, depth, width), bf16),
        in_specs=[whole()] * len(halves),
        out_specs=whole(),
        compiler_params=params(4 if mine <= 64 else 30),
        name="join",
    )(*halves)
    pieces = lax.all_to_all(partial, ("expert", "chip"), split_axis=0, concat_axis=0, tiled=True)
    return pl.pallas_call(
        mix_kernel,
        out_shape=jax.ShapeDtypeStruct((tok, width), bf16),
        in_specs=[whole()] * 2,
        out_specs=whole(),
        compiler_params=params(16),
        name="mix",
    )(meta, pieces.reshape(experts, zs, depth, width))


def solution(mesh):
    experts, shards = mesh.shape["expert"], mesh.shape["shard"]
    devices = mesh.devices.reshape(experts, shards // CORES, CORES)
    split = Mesh(devices, ("expert", "chip", "core"))
    everywhere = P(("expert", "chip", "core"), None)
    columns = P("expert", None, ("chip", "core"))
    in_specs = (
        everywhere, P(), everywhere, everywhere, P(),
        columns, columns, P("expert", ("chip", "core"), None),
    )
    return jax.shard_map(on_device, mesh=split, in_specs=in_specs, out_specs=everywhere, check_vma=False)
```
